32 devices in a mesh: dp: 1 (over z), sp: 32 (over y, x, core).
Axes of the slice: x: 4, y: 4, z: 1, core: 2. Of those that a mesh axis runs over, the one named last changes fastest.
The devices are a block of a 4x4x8 slice.
Arguments:
- hidden: bfloat16 [2, 12288, 2048], P('dp', 'sp')
- w_in: bfloat16 [2048, 6144], replicated
- w_gate: bfloat16 [2048, 4], replicated
- gate_bias: float32 [4], replicated
- a_log: float32 [4], replicated
- norm_w: float32 [2048], replicated
- w_out: bfloat16 [2048, 2048], replicated
Outputs:
- output: bfloat16 [2, 12288, 2048], P('dp', 'sp')
All inputs are finite; a program needn't handle non-finite values.
Results may differ from the reference program's by a relative error of at most 0.0109516.
Values are sent between devices in bfloat16 or wider.
A program may use at most 768 MiB of HBM per device.

```python
import jax
import jax.numpy as jnp
from jax import lax

MICRO = 2
SEQ = 12288
SHARD = 384
DMODEL = 2048
HEADS = 4
HEAD_K = 256
HEAD_V = 512
CHUNK = 64

KEY_DIM = HEADS * HEAD_K
VAL_DIM = HEADS * HEAD_V
N_CHUNKS = SEQ // CHUNK
QK_SCALE = HEAD_K ** -0.5
NORM_EPS = 1e-6


def setup_inputs(seed: int = 0, part: int = 0) -> dict:
    part_key = jax.random.fold_in(jax.random.key(seed), part)
    weight_keys = jax.random.split(jax.random.key(seed + 1), 7)
    hidden = jax.random.normal(part_key, (MICRO, SEQ, DMODEL), jnp.float32).astype(jnp.bfloat16)
    w_in = (jax.random.normal(weight_keys[0], (DMODEL, 2 * KEY_DIM + 2 * VAL_DIM), jnp.float32) * DMODEL ** -0.5).astype(jnp.bfloat16)
    w_gate = (jax.random.normal(weight_keys[1], (DMODEL, HEADS), jnp.float32) * (2.0 * DMODEL ** -0.5)).astype(jnp.bfloat16)
    gate_bias = jax.random.uniform(weight_keys[2], (HEADS,), jnp.float32, -1.0, 1.0)
    head_rates = jnp.linspace(jnp.log(0.03 / SHARD), jnp.log(0.3), HEADS)
    a_log = jax.random.permutation(weight_keys[6], head_rates) + jax.random.uniform(weight_keys[3], (HEADS,), jnp.float32, -0.5, 0.5)
    norm_w = jax.random.uniform(weight_keys[4], (VAL_DIM,), jnp.float32, 0.5, 1.5)
    w_out = (jax.random.normal(weight_keys[5], (VAL_DIM, DMODEL), jnp.float32) * VAL_DIM ** -0.5).astype(jnp.bfloat16)
    return {'hidden': hidden, 'w_in': w_in, 'w_gate': w_gate, 'gate_bias': gate_bias, 'a_log': a_log, 'norm_w': norm_w, 'w_out': w_out}


def reference(hidden, w_in, w_gate, gate_bias, a_log, norm_w, w_out):
    flat_rows = hidden.reshape(MICRO * SEQ, DMODEL)
    proj_all = jnp.dot(flat_rows, w_in, preferred_element_type=jnp.float32).astype(jnp.bfloat16)
    gate_logit = jnp.dot(flat_rows, w_gate, preferred_element_type=jnp.float32) + gate_bias
    log_decay = -jnp.exp(a_log) * jax.nn.softplus(gate_logit)

    def by_chunk(column_block, n_cols):
        return jnp.swapaxes(column_block.reshape(MICRO, N_CHUNKS, CHUNK, n_cols), 0, 1)

    queries = by_chunk(proj_all[:, :KEY_DIM], KEY_DIM)
    key_vecs = by_chunk(proj_all[:, KEY_DIM:2 * KEY_DIM], KEY_DIM)
    values = by_chunk(proj_all[:, 2 * KEY_DIM:2 * KEY_DIM + VAL_DIM], VAL_DIM)
    z_gate = by_chunk(proj_all[:, 2 * KEY_DIM + VAL_DIM:], VAL_DIM)
    decays = by_chunk(log_decay, HEADS)
    positions = jnp.arange(CHUNK)
    causal = (positions[:, None] >= positions[None, :])[None, :, :, None]
    norm_heads = norm_w.reshape(HEADS, HEAD_V)

    def chunk_step(run_state, chunk_in):
        q_chunk, k_chunk, v_chunk, z_chunk, a_chunk = chunk_in
        q_float = q_chunk.reshape(MICRO, CHUNK, HEADS, HEAD_K).astype(jnp.float32)
        k_float = k_chunk.reshape(MICRO, CHUNK, HEADS, HEAD_K).astype(jnp.float32)
        v_float = v_chunk.reshape(MICRO, CHUNK, HEADS, HEAD_V).astype(jnp.float32)
        cum_decay = jnp.cumsum(a_chunk, axis=1)
        log_gap = cum_decay[:, :, None, :] - cum_decay[:, None, :, :]
        decay_in = jnp.where(causal, jnp.exp(jnp.where(causal, log_gap, 0.0)), 0.0)
        scores = jnp.einsum('mihd,mjhd->mijh', q_float, k_float) * decay_in
        intra_term = jnp.einsum('mijh,mjhe->mihe', scores, v_float)
        inter_term = jnp.einsum('mihd,mhde->mihe', q_float, run_state) * jnp.exp(cum_decay)[..., None]
        chunk_total = cum_decay[:, -1, :]
        k_tail = k_float * jnp.exp(chunk_total[:, None, :] - cum_decay)[..., None]
        new_state = run_state * jnp.exp(chunk_total)[:, :, None, None] + jnp.einsum('mjhd,mjhe->mhde', k_tail, v_float)
        attn_out = (intra_term + inter_term) * QK_SCALE
        normed = attn_out * lax.rsqrt(jnp.mean(attn_out * attn_out, axis=-1, keepdims=True) + NORM_EPS) * norm_heads
        gated_out = normed.reshape(MICRO, CHUNK, VAL_DIM) * jax.nn.silu(z_chunk.astype(jnp.float32))
        return new_state, gated_out.astype(jnp.bfloat16)

    init_state = jnp.zeros((MICRO, HEADS, HEAD_K, HEAD_V), jnp.float32)
    _, gated_all = lax.scan(chunk_step, init_state, (queries, key_vecs, values, z_gate, decays))
    gated_rows = jnp.swapaxes(gated_all, 0, 1).reshape(MICRO * SEQ, VAL_DIM)
    result = jnp.dot(gated_rows, w_out, preferred_element_type=jnp.float32).astype(jnp.bfloat16)
    return result.reshape(MICRO, SEQ, DMODEL)
```

```python
import functools

import jax
import jax.numpy as jnp
from jax import lax
from jax.experimental import pallas as pl
from jax.experimental.pallas import tpu as pltpu
from jax.sharding import PartitionSpec as P

NORM_EPS = 1e-6
CORES = 2
PIECES = 16
LAG = 4
MESH = pl.DeviceIdType.MESH
F32 = jnp.float32
BF16 = jnp.bfloat16


def chip_grid(chips):
    nx = int(chips ** 0.5)
    while chips % nx:
        nx -= 1
    return chips // nx, nx


def layer_kernel(ny, nx, hidden, w_in, w_gate, gate_bias, a_log, norm_w, w_out, out,
                 x_v, w_v, wo_v, wg_v, par_v, proj, intra, acc, y_v,
                 cl, clt, etail, ecum, dtile, dbuf, coef,
                 state, c_in, f_in, g_in, c_out, f_out, g_out,
                 x_sem, xs_sem, xr_sem, w_sem, wo_sem, ds_sem, dr_sem, send_sem, recv_sem, o_sem, os_sem, or_sem):
    rows = hidden.shape[1]
    n_heads = w_gate.shape[1]
    val_dim = w_out.shape[0]
    key_dim = (w_in.shape[1] - 2 * val_dim) // 2
    head_k, head_v = key_dim // n_heads, val_dim // n_heads
    blk = head_k + head_v
    tiles = blk // head_k
    total = n_heads * PIECES
    prow = head_k // 8 // PIECES
    hrow = head_k // 8

    me = lax.axis_index('sp')
    core = lax.rem(me, CORES)
    chip = lax.div(me, CORES)
    x = lax.rem(chip, nx)
    y = lax.div(chip, nx)

    def device(yy, xx, cc):
        return {'sp': (yy * nx + xx) * CORES + cc}

    partner = device(y, x, 1 - core)
    down = device(lax.rem(y + 1, ny), x, core)
    up = device(lax.rem(y + ny - 1, ny), x, core)
    right = device(y, lax.rem(x + 1, nx), core)
    left = device(y, lax.rem(x + nx - 1, nx), core)

    def mate(offset):
        return device(y, lax.rem(x + offset, nx), core)

    x_load = pltpu.make_async_copy(hidden.at[core], x_v.at[core], x_sem)
    x_load.start()

    def w_copies(seq, is_kv, h):
        slot = lax.rem(seq, 3)
        k_at = jnp.where(is_kv, key_dim, 0) + h * head_k
        v_at = 2 * key_dim + jnp.where(is_kv, 0, val_dim) + h * head_v
        return (
            pltpu.make_async_copy(w_in.at[:, pl.ds(pl.multiple_of(k_at, 128), head_k)], w_v.at[slot, :, 0:head_k], w_sem.at[slot, 0]),
            pltpu.make_async_copy(w_in.at[:, pl.ds(pl.multiple_of(v_at, 128), head_v)], w_v.at[slot, :, head_k:blk], w_sem.at[slot, 1]),
        )

    def w_start(seq, is_kv, h):
        for copy in w_copies(seq, is_kv, h):
            copy.start()

    def w_wait(seq, is_kv, h):
        for copy in w_copies(seq, is_kv, h):
            copy.wait()

    def wo_copy(h):
        slot = lax.rem(h, 2)
        return pltpu.make_async_copy(w_out.at[pl.ds(pl.multiple_of(h * head_v, 128), head_v), :], wo_v.at[slot], wo_sem.at[slot])

    w_start(0, True, 0)

    barrier = pltpu.get_barrier_semaphore()
    peers = [partner, down, up] + [mate(o) for o in range(1, nx)]
    for peer in peers:
        pl.semaphore_signal(barrier, inc=1, device_id=peer, device_id_type=MESH)
    pl.semaphore_wait(barrier, len(peers))

    x_send = pltpu.make_async_remote_copy(hidden.at[1 - core], x_v.at[core], xs_sem, xr_sem, device_id=partner, device_id_type=MESH)
    x_send.start()
    x_recv = pltpu.make_async_remote_copy(hidden.at[1 - core], x_v.at[1 - core], xs_sem, xr_sem, device_id=partner, device_id_type=MESH)
    w_start(1, True, 1)
    w_start(2, False, 0)

    wg_v[...] = jnp.zeros_like(wg_v)
    wg_v[:, 0:n_heads] = w_gate[...]
    par_v[...] = jnp.zeros_like(par_v)
    par_v[0:1, 0:n_heads] = gate_bias[...]
    par_v[8:9, 0:n_heads] = a_log[...]

    @pl.when(y == 0)
    def _():
        c_in[...] = jnp.zeros_like(c_in)
        g_in[...] = jnp.zeros_like(g_in)

    @pl.when(jnp.logical_and(y > 0, x == nx - 1))
    def _():
        g_in[...] = jnp.zeros_like(g_in)

    @pl.when(x == 0)
    def _():
        f_in[...] = jnp.zeros_like(f_in)

    lane = lax.broadcasted_iota(jnp.int32, (1, 128), 1)

    def gate_half(b):
        logit = jnp.dot(x_v[b], wg_v[...], preferred_element_type=F32) + par_v[0:1, :]
        soft = jnp.maximum(logit, 0.0) + jnp.log1p(jnp.exp(-jnp.abs(logit)))
        decay = -jnp.exp(par_v[8:9, :]) * soft
        tri = lax.broadcasted_iota(jnp.int32, (rows, rows), 0) >= lax.broadcasted_iota(jnp.int32, (rows, rows), 1)
        cum = jnp.dot(jnp.where(tri, 1.0, 0.0).astype(F32), decay, precision=lax.Precision.HIGHEST, preferred_element_type=F32)
        cl[b] = cum
        clt[b] = jnp.transpose(cum)

    def proj_half(b):
        def one(j, carry):
            cols = pl.ds(pl.multiple_of(j * head_k, 128), head_k)
            part = jnp.dot(x_v[b], w_v[0, :, cols], preferred_element_type=F32)
            proj[0, b, :, cols] = part.astype(BF16)
            return carry
        lax.fori_loop(0, tiles, one, 0)

    x_load.wait()
    gate_half(core)
    w_wait(0, True, 0)
    proj_half(core)
    x_recv.wait_recv()
    gate_half(1 - core)

    tot0 = cl[0, rows - 1:rows, :]
    tot1 = cl[1, rows - 1:rows, :]
    own = jnp.broadcast_to(tot0 + tot1, (8, 128))
    dtile[...] = own
    dbuf[x] = own

    def d_copy(offset, source):
        return pltpu.make_async_remote_copy(dtile, dbuf.at[source], ds_sem.at[offset - 1], dr_sem.at[offset - 1], device_id=mate(offset), device_id_type=MESH)

    for o in range(1, nx):
        d_copy(o, x).start()
    etail[0] = jnp.exp((tot0 - cl[0]) + tot1)
    etail[1] = jnp.exp(tot1 - cl[1])
    ecum[0] = jnp.exp(cl[0])
    ecum[1] = jnp.exp(cl[1] + tot0)
    proj_half(1 - core)
    w_start(3, True, 2)
    wo_copy(0).start()
    wo_copy(1).start()

    def column(ref, b, h):
        return jnp.sum(jnp.where(lane == h, ref[b], 0.0), axis=1, keepdims=True)

    def row_of(b, h):
        sub = lax.broadcasted_iota(jnp.int32, (8, 1), 0)
        return jnp.sum(jnp.where(sub == h, clt[b, 0:8, :], 0.0), axis=0, keepdims=True)

    def chip_state(h):
        out_sum = None
        for b in range(2):
            keys = proj[h, b, :, 0:head_k].astype(F32) * column(etail, b, h)
            vals = proj[h, b, :, head_k:blk].astype(F32)
            part = lax.dot_general(keys, vals, (((0,), (0,)), ((), ())), preferred_element_type=F32)
            out_sum = part if out_sum is None else out_sum + part
        state[pl.ds(h * hrow, hrow)] = out_sum.reshape(hrow, 8, head_v)

    chip_state(0)
    for o in range(1, nx):
        d_copy(o, lax.rem(x + nx - o, nx)).wait_recv()
    logs = [dbuf[i] for i in range(nx)]
    zero = jnp.zeros((8, 128), F32)
    log_row, log_start, log_end = zero, zero, zero
    for i in range(nx):
        log_row = log_row + logs[i]
        log_start = log_start + jnp.where(i < x, logs[i], 0.0)
        log_end = log_end + jnp.where(i > x, logs[i], 0.0)
    for kind, log_w in enumerate((own, log_start, log_end, log_row)):
        for h in range(n_heads):
            one = jnp.sum(jnp.where(lane == h, log_w, 0.0), axis=1, keepdims=True)
            coef[kind, h] = jnp.broadcast_to(jnp.exp(one), (8, head_v))

    def piece(ref, p):
        return ref.at[pl.ds(p * prow, prow)]

    def flow(kind, src, dst, p, target):
        return pltpu.make_async_remote_copy(piece(src, p), piece(dst, p), send_sem.at[kind, p], recv_sem.at[kind, p], device_id=target, device_id_type=MESH)

    c_sends, c_recvs = y < ny - 1, y > 0
    f_sends, f_recvs = x < nx - 1, x > 0
    g_sends, g_recvs = jnp.logical_and(y > 0, x > 0), jnp.logical_and(y > 0, x < nx - 1)

    def comm(s):
        def at(lag):
            p = s - lag * LAG
            return p, jnp.logical_and(p >= 0, p < total)

        p, live = at(y)

        @pl.when(jnp.logical_and(live, c_recvs))
        def _(p=p):
            flow(0, c_out, c_in, p, down).wait_recv()

        @pl.when(jnp.logical_and(live, c_sends))
        def _(p=p):
            h = lax.div(p, PIECES)
            at_p = pl.ds(p * prow, prow)
            c_out[at_p] = coef[3, h] * c_in[at_p] + coef[2, h] * state[at_p]
            flow(0, c_out, c_in, p, down).start()

        p, live = at(y + x)

        @pl.when(jnp.logical_and(live, f_recvs))
        def _(p=p):
            flow(1, f_out, f_in, p, right).wait_recv()

        @pl.when(jnp.logical_and(live, f_sends))
        def _(p=p):
            h = lax.div(p, PIECES)
            at_p = pl.ds(p * prow, prow)
            f_out[at_p] = coef[0, h] * (f_in[at_p] + coef[1, h] * c_in[at_p]) + state[at_p]
            flow(1, f_out, f_in, p, right).start()

        p, live = at(y + nx - 1 - x)

        @pl.when(jnp.logical_and(live, g_recvs))
        def _(p=p):
            flow(2, g_out, g_in, p, left).wait_recv()

        @pl.when(jnp.logical_and(live, g_sends))
        def _(p=p):
            at_p = pl.ds(p * prow, prow)
            g_out[at_p] = g_in[at_p] + c_in[at_p]
            flow(2, g_out, g_in, p, left).start()

        p, live = at(y + jnp.maximum(x, nx - 1 - x))

        @pl.when(live)
        def _(p=p):
            h = lax.div(p, PIECES)
            at_p = pl.ds(p * prow, prow)
            state[at_p] = f_in[at_p] + coef[1, h] * (c_in[at_p] + g_in[at_p])

    def comm_steps(s, n):
        lax.fori_loop(0, n, lambda i, c: (comm(s + i), c)[1], 0)

    def proj_tile(seq, dest, j):
        slot = lax.rem(seq, 3)
        cols = pl.ds(pl.multiple_of(j * head_k, 128), head_k)
        rows_all = x_v[...].reshape(2 * rows, x_v.shape[2])
        part = jnp.dot(rows_all, w_v[slot, :, cols], preferred_element_type=F32)
        proj[dest, :, :, cols] = part.astype(BF16).reshape(2, rows, head_k)

    def intra_block(h, b):
        q = proj[n_heads + h, b, :, 0:head_k]
        cum_i = column(cl, b, h)
        causal = lax.broadcasted_iota(jnp.int32, (rows, rows), 0) >= lax.broadcasted_iota(jnp.int32, (rows, rows), 1)
        o = None
        for src in range(b + 1):
            keys = proj[h, src, :, 0:head_k]
            vals = proj[h, src, :, head_k:blk].astype(F32)
            score = lax.dot_general(q, keys, (((1,), (1,)), ((), ())), preferred_element_type=F32)
            cum_j = row_of(src, h)
            if src == b:
                weight = jnp.where(causal, jnp.exp(jnp.where(causal, cum_i - cum_j, 0.0)), 0.0)
            else:
                weight = jnp.exp(cum_i + (cum_j[:, rows - 1:rows] - cum_j))
            part = jnp.dot(score * weight, vals, preferred_element_type=F32)
            o = part if o is None else o + part
        intra[h, b] = o

    half_rows = rows // 6
    scale = head_k ** -0.5

    def finish_half(h, b, last):
        q = proj[n_heads + h, b, :, 0:head_k].astype(F32)
        entering = state[pl.ds(h * hrow, hrow)].reshape(head_k, head_v)
        inter = jnp.dot(q, entering, preferred_element_type=F32) * column(ecum, b, h)
        intra[h, b] = (intra[h, b] + inter) * scale
        gain = norm_w[0:1, pl.ds(pl.multiple_of(h * head_v, 128), head_v)]

        def norm(i, carry):
            at_r = pl.ds(pl.multiple_of(i * half_rows, 16), half_rows)
            o = intra[h, b, at_r, :]
            z = proj[n_heads + h, b, at_r, head_k:blk].astype(F32)
            n = o * lax.rsqrt(jnp.mean(o * o, axis=1, keepdims=True) + NORM_EPS) * gain
            y_v[at_r, :] = (n * (z / (1.0 + jnp.exp(-z)))).astype(BF16)
            return carry
        lax.fori_loop(0, rows // half_rows, norm, 0)

        def project(j, carry):
            cols = pl.ds(pl.multiple_of(j * head_v, 128), head_v)
            part = jnp.dot(y_v[...], wo_v[lax.rem(h, 2), :, cols], preferred_element_type=F32)
            if last:
                x_v[b, :, cols] = (acc[b, :, cols] + part).astype(BF16)
            else:
                acc[b, :, cols] = acc[b, :, cols] + part
            return carry
        lax.fori_loop(0, w_out.shape[1] // head_v, project, 0)

    per = PIECES // 8

    def round_body(h, carry):
        s0 = (h - 1) * PIECES
        w_wait(2 * h - 1, True, h)

        def kv_tile(j, c):
            proj_tile(2 * h - 1, h, j)
            comm_steps(s0 + j * per, per)
            return c
        lax.fori_loop(0, tiles, kv_tile, 0)
        w_start(2 * h + 2, False, h)
        chip_state(h)
        comm_steps(s0 + 3 * per, per)
        w_wait(2 * h, False, h - 1)

        def qz_tile(j, c):
            proj_tile(2 * h, n_heads + h - 1, j)
            comm_steps(s0 + (4 + j) * per, per)
            return c
        lax.fori_loop(0, tiles, qz_tile, 0)

        @pl.when(h == 1)
        def _():
            w_start(2 * h + 3, True, h + 2)
        intra_block(h - 1, 0)
        comm_steps(s0 + 7 * per, per)
        intra_block(h - 1, 1)
        return carry
    lax.fori_loop(1, n_heads, round_body, 0)

    last_head = n_heads - 1
    lags = (ny - 1 + nx - 1) * LAG
    s1 = last_head * PIECES
    w_wait(2 * n_heads, False, last_head)
    acc[...] = jnp.zeros_like(acc)
    each = lags // 8

    def last_tile(j, c):
        proj_tile(2 * n_heads, n_heads + last_head, j)
        comm_steps(s1 + j * each, each)
        return c
    lax.fori_loop(0, tiles, last_tile, 0)
    intra_block(last_head, 0)
    comm_steps(s1 + 3 * each, each)
    intra_block(last_head, 1)

    def early(i, c):
        h = lax.div(i, 2)

        @pl.when(lax.rem(i, 2) == 0)
        def _():
            wo_copy(h).wait()
        finish_half(h, lax.rem(i, 2), False)

        @pl.when(jnp.logical_and(lax.rem(i, 2) == 1, h + 2 < n_heads))
        def _():
            wo_copy(h + 2).start()
        n = jnp.where(i < 3, each, jnp.where(i == 3, lags - 7 * each, 2))
        at_s = s1 + jnp.where(i < 4, (4 + i) * each, lags + (i - 4) * 2)
        lax.fori_loop(0, n, lambda k, cc: (comm(at_s + k), cc)[1], 0)
        return c
    lax.fori_loop(0, 2 * last_head, early, 0)
    done = lags + (2 * last_head - 4) * 2
    comm_steps(s1 + done, total + lags - s1 - done)

    wo_copy(last_head).wait()
    finish_half(last_head, 1 - core, True)
    o_send = pltpu.make_async_remote_copy(x_v.at[1 - core], out.at[core], os_sem, or_sem, device_id=partner, device_id_type=MESH)
    o_send.start()
    finish_half(last_head, core, True)
    o_store = pltpu.make_async_copy(x_v.at[core], out.at[core], o_sem)
    o_store.start()

    x_send.wait_send()
    for o in range(1, nx):
        d_copy(o, x).wait_send()

    def drain(p, c):
        @pl.when(c_sends)
        def _():
            flow(0, c_out, c_in, p, down).wait_send()

        @pl.when(f_sends)
        def _():
            flow(1, f_out, f_in, p, right).wait_send()

        @pl.when(g_sends)
        def _():
            flow(2, g_out, g_in, p, left).wait_send()
        return c
    lax.fori_loop(0, total, drain, 0)
    o_store.wait()
    o_send.wait_send()
    pltpu.make_async_remote_copy(x_v.at[1 - core], out.at[1 - core], os_sem, or_sem, device_id=partner, device_id_type=MESH).wait_recv()


def solution(mesh):
    ny, nx = chip_grid(mesh.shape['sp'] // CORES)

    def device_body(hidden, w_in, w_gate, gate_bias, a_log, norm_w, w_out):
        _, rows, d_model = hidden.shape
        n_heads = w_gate.shape[1]
        val_dim = w_out.shape[0]
        key_dim = (w_in.shape[1] - 2 * val_dim) // 2
        head_k, head_v = key_dim // n_heads, val_dim // n_heads
        blk = head_k + head_v
        total = n_heads * PIECES
        any_space = pl.BlockSpec(memory_space=pl.ANY)
        vmem = pl.BlockSpec(memory_space=pltpu.VMEM)
        flow_buf = pltpu.VMEM((n_heads * head_k // 8, 8, head_v), F32)
        dma = pltpu.SemaphoreType.DMA
        return pl.pallas_call(
            functools.partial(layer_kernel, ny, nx),
            out_shape=jax.ShapeDtypeStruct(hidden.shape, BF16),
            in_specs=[any_space, any_space, vmem, vmem, vmem, vmem, any_space],
            out_specs=any_space,
            scratch_shapes=[
                pltpu.VMEM((2, rows, d_model), BF16),
                pltpu.VMEM((3, d_model, blk), BF16),
                pltpu.VMEM((2, head_v, w_out.shape[1]), BF16),
                pltpu.VMEM((d_model, 128), BF16),
                pltpu.VMEM((16, 128), F32),
                pltpu.VMEM((2 * n_heads, 2, rows, blk), BF16),
                pltpu.VMEM((n_heads, 2, rows, head_v), F32),
                pltpu.VMEM((2, rows, w_out.shape[1]), F32),
                pltpu.VMEM((rows, head_v), BF16),
                pltpu.VMEM((2, rows, 128), F32),
                pltpu.VMEM((2, 128, rows), F32),
                pltpu.VMEM((2, rows, 128), F32),
                pltpu.VMEM((2, rows, 128), F32),
                pltpu.VMEM((8, 128), F32),
                pltpu.VMEM((nx, 8, 128), F32),
                pltpu.VMEM((4, n_heads, 8, head_v), F32),
                flow_buf, flow_buf, flow_buf, flow_buf, flow_buf, flow_buf, flow_buf,
                dma, dma, dma, dma((3, 2)), dma((2,)), dma((nx - 1,)), dma((nx - 1,)),
                dma((3, total)), dma((3, total)), dma, dma, dma,
            ],
            compiler_params=pltpu.CompilerParams(collective_id=0, has_side_effects=True, vmem_limit_bytes=67043328),
        )(hidden, w_in, w_gate, gate_bias.reshape(1, -1), a_log.reshape(1, -1), norm_w.reshape(1, -1), w_out)

    return jax.shard_map(device_body, mesh=mesh, in_specs=(P('dp', 'sp', None), P(), P(), P(), P(), P(), P()), out_specs=P('dp', 'sp', None), check_vma=False)
```

```python
import functools

import jax
import jax.numpy as jnp
from jax import lax
from jax.experimental import pallas as pl
from jax.experimental.pallas import tpu as pltpu
from jax.sharding import PartitionSpec as P

NORM_EPS = 1e-6
CORES = 2
PIECES = 8
LAG = 3
MESH = pl.DeviceIdType.MESH
F32 = jnp.float32
BF16 = jnp.bfloat16


def chip_grid(chips):
    nx = int(chips ** 0.5)
    while chips % nx:
        nx -= 1
    return chips // nx, nx


def layer_kernel(ny, nx, hidden, w_in, w_gate, gate_bias, a_log, norm_w, w_out, out,
                 x_v, w_v, wo_v, wg_v, par_v, proj, intra, acc, y_v,
                 cl, clt, etail, ecum, dtile, dbuf, coef,
                 state, c_in, f_in, g_in, c_out, f_out, g_out,
                 x_sem, xs_sem, xr_sem, w_sem, wo_sem, ds_sem, dr_sem, send_sem, recv_sem, o_sem, os_sem, or_sem):
    rows = hidden.shape[1]
    n_heads = w_gate.shape[0]
    val_dim = w_out.shape[0]
    key_dim = (w_in.shape[1] - 2 * val_dim) // 2
    head_k, head_v = key_dim // n_heads, val_dim // n_heads
    blk = head_k + head_v
    tiles = blk // head_k
    total = n_heads * PIECES
    prow = head_k // 8 // PIECES
    hrow = head_k // 8

    me = lax.axis_index('sp')
    core = lax.rem(me, CORES)
    chip = lax.div(me, CORES)
    x = lax.rem(chip, nx)
    y = lax.div(chip, nx)

    def device(yy, xx, cc):
        return {'sp': (yy * nx + xx) * CORES + cc}

    partner = device(y, x, 1 - core)
    down = device(lax.rem(y + 1, ny), x, core)
    up = device(lax.rem(y + ny - 1, ny), x, core)
    right = device(y, lax.rem(x + 1, nx), core)
    left = device(y, lax.rem(x + nx - 1, nx), core)

    def mate(offset):
        return device(y, lax.rem(x + offset, nx), core)

    x_load = pltpu.make_async_copy(hidden.at[core], x_v.at[core], x_sem)
    x_load.start()

    def w_copies(seq, is_kv, h):
        slot = lax.rem(seq, 3)
        k_at = jnp.where(is_kv, key_dim, 0) + h * head_k
        v_at = 2 * key_dim + jnp.where(is_kv, 0, val_dim) + h * head_v
        return (
            pltpu.make_async_copy(w_in.at[:, pl.ds(pl.multiple_of(k_at, 128), head_k)], w_v.at[slot, :, 0:head_k], w_sem.at[slot, 0]),
            pltpu.make_async_copy(w_in.at[:, pl.ds(pl.multiple_of(v_at, 128), head_v)], w_v.at[slot, :, head_k:blk], w_sem.at[slot, 1]),
        )

    def kv_seq(h):
        return jnp.maximum(2 * h - 1, 0)

    def qz_seq(h):
        return 2 * h + 2

    def w_start(seq, is_kv, h):
        for copy in w_copies(seq, is_kv, h):
            copy.start()

    def w_wait(seq, is_kv, h):
        for copy in w_copies(seq, is_kv, h):
            copy.wait()

    def wo_copy(h):
        slot = lax.rem(h, 2)
        return pltpu.make_async_copy(w_out.at[pl.ds(pl.multiple_of(h * head_v, 128), head_v), :], wo_v.at[slot], wo_sem.at[slot])

    w_start(kv_seq(0), True, 0)

    barrier = pltpu.get_barrier_semaphore()
    peers = [partner, down, up] + [mate(o) for o in range(1, nx)]
    for peer in peers:
        pl.semaphore_signal(barrier, inc=1, device_id=peer, device_id_type=MESH)
    wg_v[...] = jnp.zeros_like(wg_v)
    wg_v[0:n_heads, :] = w_gate[...]
    par_v[...] = jnp.zeros_like(par_v)
    par_v[0:1, 0:n_heads] = gate_bias[...]
    par_v[8:9, 0:n_heads] = a_log[...]
    pl.semaphore_wait(barrier, len(peers))

    x_send = pltpu.make_async_remote_copy(hidden.at[1 - core], x_v.at[core], xs_sem, xr_sem, device_id=partner, device_id_type=MESH)
    x_send.start()
    x_recv = pltpu.make_async_remote_copy(hidden.at[1 - core], x_v.at[1 - core], xs_sem, xr_sem, device_id=partner, device_id_type=MESH)
    w_start(kv_seq(1), True, 1)
    w_start(qz_seq(0), False, 0)

    lane = lax.broadcasted_iota(jnp.int32, (1, 128), 1)
    tri = (lax.broadcasted_iota(jnp.int32, (128, 128), 0) >= lax.broadcasted_iota(jnp.int32, (128, 128), 1))

    def gate_half(b):
        logit = lax.dot_general(x_v[b], wg_v[...], (((1,), (1,)), ((), ())), preferred_element_type=F32) + par_v[0:1, :]
        soft = jnp.maximum(logit, 0.0) + jnp.log1p(jnp.exp(-jnp.abs(logit)))
        cl[b] = -jnp.exp(par_v[8:9, :]) * soft
        ones = jnp.where(tri, 1.0, 0.0).astype(BF16)

        def run(i, before):
            at_r = pl.ds(pl.multiple_of(i * 128, 128), 128)
            decay = cl[b, at_r, :]
            top = decay.astype(BF16)
            rest = decay - top.astype(F32)
            mid = rest.astype(BF16)
            low = (rest - mid.astype(F32)).astype(BF16)
            sums = jnp.dot(ones, jnp.concatenate([top, mid, low], axis=1), preferred_element_type=F32)
            cum = before + (sums[:, 0:128] + (sums[:, 128:256] + sums[:, 256:384]))
            cl[b, at_r, :] = cum
            clt[b, :, at_r] = jnp.transpose(cum)
            return cum[127:128, :]
        lax.fori_loop(0, rows // 128, run, jnp.zeros((1, 128), F32))

    def proj_half(seq, dest, j, b):
        cols = pl.ds(pl.multiple_of(j * head_k, 128), head_k)
        part = jnp.dot(x_v[b], w_v[lax.rem(seq, 3), :, cols], preferred_element_type=F32)
        proj[dest, b, :, cols] = part.astype(BF16)

    def d_copy(offset, source):
        return pltpu.make_async_remote_copy(dtile, dbuf.at[source], ds_sem.at[offset - 1], dr_sem.at[offset - 1], device_id=mate(offset), device_id_type=MESH)

    def chip_decays():
        tot0 = cl[0, rows - 1:rows, :]
        tot1 = cl[1, rows - 1:rows, :]
        own = jnp.broadcast_to(tot0 + tot1, (8, 128))
        dtile[...] = own
        dbuf[x] = own
        for o in range(1, nx):
            d_copy(o, x).start()

        def powers(i, carry):
            at_r = pl.ds(pl.multiple_of(i * 64, 64), 64)
            etail[0, at_r, :] = jnp.exp((tot0 - cl[0, at_r, :]) + tot1)
            etail[1, at_r, :] = jnp.exp(tot1 - cl[1, at_r, :])
            ecum[0, at_r, :] = jnp.exp(cl[0, at_r, :])
            ecum[1, at_r, :] = jnp.exp(cl[1, at_r, :] + tot0)
            return carry
        lax.fori_loop(0, rows // 64, powers, 0)

    def column(ref, b, h):
        return jnp.sum(jnp.where(lane == h, ref[b], 0.0), axis=1, keepdims=True)

    def row_of(b, h):
        sub = lax.broadcasted_iota(jnp.int32, (8, 1), 0)
        return jnp.sum(jnp.where(sub == h, clt[b, 0:8, :], 0.0), axis=0, keepdims=True)

    def chip_state(h):
        out_sum = None
        for b in range(2):
            keys = proj[h, b, :, 0:head_k].astype(F32) * column(etail, b, h)
            vals = proj[h, b, :, head_k:blk].astype(F32)
            part = lax.dot_general(keys, vals, (((0,), (0,)), ((), ())), preferred_element_type=F32)
            out_sum = part if out_sum is None else out_sum + part
        state[pl.ds(h * hrow, hrow)] = out_sum.reshape(hrow, 8, head_v)

    def row_weights():
        for o in range(1, nx):
            d_copy(o, lax.rem(x + nx - o, nx)).wait_recv()
        zero = jnp.zeros((8, 128), F32)
        log_row, log_start, log_end = zero, zero, zero
        for i in range(nx):
            log_i = dbuf[i]
            log_row = log_row + log_i
            log_start = log_start + jnp.where(i < x, log_i, 0.0)
            log_end = log_end + jnp.where(i > x, log_i, 0.0)
        for kind, log_w in enumerate((dtile[...], log_start, log_end, log_row)):
            for h in range(n_heads):
                one = jnp.sum(jnp.where(lane == h, log_w, 0.0), axis=1, keepdims=True)
                coef[kind, h] = jnp.broadcast_to(jnp.exp(one), (8, head_v))

    def piece(ref, p):
        return ref.at[pl.ds(p * prow, prow)]

    def flow(kind, src, dst, p, target):
        return pltpu.make_async_remote_copy(piece(src, p), piece(dst, p), send_sem.at[kind, p], recv_sem.at[kind, p], device_id=target, device_id_type=MESH)

    c_sends, c_recvs = y < ny - 1, y > 0
    f_sends, f_recvs = x < nx - 1, x > 0
    g_sends, g_recvs = jnp.logical_and(y > 0, x > 0), jnp.logical_and(y > 0, x < nx - 1)

    def comm(s):
        def at(lag):
            p = s - lag * LAG
            return p, jnp.logical_and(p >= 0, p < total)

        def arrive(live, recvs, p, ref, copy):
            @pl.when(jnp.logical_and(live, recvs))
            def _():
                copy.wait_recv()

            @pl.when(jnp.logical_and(live, jnp.logical_not(recvs)))
            def _():
                ref[pl.ds(p * prow, prow)] = jnp.zeros((prow, 8, head_v), F32)

        p, live = at(y)
        arrive(live, c_recvs, p, c_in, flow(0, c_out, c_in, p, down))

        @pl.when(jnp.logical_and(live, c_sends))
        def _(p=p):
            h = lax.div(p, PIECES)
            at_p = pl.ds(p * prow, prow)
            c_out[at_p] = coef[3, h] * c_in[at_p] + coef[2, h] * state[at_p]
            flow(0, c_out, c_in, p, down).start()

        p, live = at(y + x)
        arrive(live, f_recvs, p, f_in, flow(1, f_out, f_in, p, right))

        @pl.when(jnp.logical_and(live, f_sends))
        def _(p=p):
            h = lax.div(p, PIECES)
            at_p = pl.ds(p * prow, prow)
            f_out[at_p] = coef[0, h] * (f_in[at_p] + coef[1, h] * c_in[at_p]) + state[at_p]
            flow(1, f_out, f_in, p, right).start()

        p, live = at(y + nx - 1 - x)
        arrive(live, g_recvs, p, g_in, flow(2, g_out, g_in, p, left))

        @pl.when(jnp.logical_and(live, g_sends))
        def _(p=p):
            at_p = pl.ds(p * prow, prow)
            g_out[at_p] = g_in[at_p] + c_in[at_p]
            flow(2, g_out, g_in, p, left).start()

        p, live = at(y + jnp.maximum(x, nx - 1 - x))

        @pl.when(live)
        def _(p=p):
            h = lax.div(p, PIECES)
            at_p = pl.ds(p * prow, prow)
            state[at_p] = f_in[at_p] + coef[1, h] * (c_in[at_p] + g_in[at_p])

    def score_block(h, b, src):
        same = src == b
        q = proj[n_heads + h, b, :, 0:head_k]
        keys = proj[h, src, :, 0:head_k]
        score = lax.dot_general(q, keys, (((1,), (1,)), ((), ())), preferred_element_type=F32)
        cum_i = column(cl, b, h)
        cum_j = row_of(src, h)
        rest = jnp.where(same, -cum_j, cum_j[:, rows - 1:rows] - cum_j)
        ahead = lax.broadcasted_iota(jnp.int32, (rows, rows), 1) - lax.broadcasted_iota(jnp.int32, (rows, rows), 0)
        causal = ahead <= jnp.where(same, 0, rows)
        weight = jnp.where(causal, jnp.exp(jnp.where(causal, cum_i + rest, 0.0)), 0.0)
        vals = proj[h, src, :, head_k:blk].astype(F32)
        part = jnp.dot(score * weight, vals, preferred_element_type=F32)
        intra[h, b] = jnp.where(src == 0, 0.0, intra[h, b]) + part

    nrow = 64
    scale = head_k ** -0.5

    def finish_half(h, b):
        q = proj[n_heads + h, b, :, 0:head_k].astype(F32)
        entering = state[pl.ds(h * hrow, hrow)].reshape(head_k, head_v)
        inter = jnp.dot(q, entering, preferred_element_type=F32) * column(ecum, b, h)
        intra[h, b] = (intra[h, b] + inter) * scale
        gain = norm_w[0:1, pl.ds(pl.multiple_of(h * head_v, 128), head_v)]

        def norm(i, carry):
            at_r = pl.ds(pl.multiple_of(i * nrow, nrow), nrow)
            o = intra[h, b, at_r, :]
            z = proj[n_heads + h, b, at_r, head_k:blk].astype(F32)
            n = o * lax.rsqrt(jnp.mean(o * o, axis=1, keepdims=True) + NORM_EPS) * gain
            y_v[at_r, :] = (n * (z / (1.0 + jnp.exp(-z)))).astype(BF16)
            return carry
        lax.fori_loop(0, rows // nrow, norm, 0)

        def project(j, carry):
            cols = pl.ds(pl.multiple_of(j * head_v, 128), head_v)
            part = jnp.dot(y_v[...], wo_v[lax.rem(h, 2), :, cols], preferred_element_type=F32)
            new = jnp.where(h > 0, acc[b, :, cols], 0.0) + part
            acc[b, :, cols] = new
            x_v[b, :, cols] = new.astype(BF16)
            return carry
        lax.fori_loop(0, w_out.shape[1] // head_v, project, 0)

    o_send = pltpu.make_async_remote_copy(x_v.at[1 - core], out.at[core], os_sem, or_sem, device_id=partner, device_id_type=MESH)
    o_store = pltpu.make_async_copy(x_v.at[core], out.at[core], o_sem)

    per = 2 * tiles
    at_state, at_qz = per, per + 1
    at_score = at_qz + per
    at_fin = at_score + 3
    first_fins = 2 * (n_heads - 2)
    ends = at_fin + first_fins
    lags = (ny - 1 + nx - 1) * LAG
    last = n_heads - 1

    def slot_body(r, u):
        start = r == 0
        fin_round = r >= n_heads

        @pl.when(jnp.logical_and(start, u == 0))
        def _():
            x_load.wait()

        @pl.when(jnp.logical_and(start, u == tiles))
        def _():
            x_recv.wait_recv()

        @pl.when(jnp.logical_and(start, jnp.logical_or(u == 0, u == tiles)))
        def _():
            gate_half(jnp.where(u == 0, core, 1 - core))

        @pl.when(jnp.logical_and(start, u == tiles))
        def _():
            chip_decays()

        @pl.when(u == 0)
        def _():
            w_wait(kv_seq(r), True, r)

        @pl.when(u == at_qz)
        def _():
            w_wait(qz_seq(r - 1), False, r - 1)

        is_kv = u < at_state

        @pl.when(jnp.logical_or(is_kv, jnp.logical_and(u >= at_qz, u < at_score)))
        def _():
            v = jnp.where(is_kv, u, u - at_qz)
            b = jnp.where(v < tiles, core, 1 - core)
            seq = jnp.where(is_kv, kv_seq(r), qz_seq(r - 1))
            proj_half(seq, jnp.where(is_kv, r, n_heads + r - 1), lax.rem(v, tiles), b)

        @pl.when(u == at_state)
        def _():
            fetch_kv = start
            w_start(jnp.where(fetch_kv, kv_seq(2), qz_seq(r)), fetch_kv, jnp.where(fetch_kv, 2, r))
            chip_state(r)

        @pl.when(jnp.logical_and(start, u == at_state))
        def _():
            row_weights()

        @pl.when(jnp.logical_and(r == 1, u == at_score))
        def _():
            w_start(kv_seq(3), True, 3)
            wo_copy(0).start()
            wo_copy(1).start()

        @pl.when(jnp.logical_and(u >= at_score, u < at_fin))
        def _():
            v = u - at_score
            score_block(r - 1, jnp.where(v == 0, 0, 1), jnp.where(v == 2, 1, 0))

        @pl.when(u >= at_fin)
        def _():
            v = u - at_fin
            h = jnp.where(r == n_heads, lax.div(v, 2), r - 3)
            second = lax.rem(v, 2)

            @pl.when(second == 0)
            def _():
                wo_copy(h).wait()
            finish_half(h, jnp.where(second == 0, 1 - core, core))

            @pl.when(jnp.logical_and(second == 1, h + 2 < n_heads))
            def _():
                wo_copy(h + 2).start()

            @pl.when(jnp.logical_and(second == 0, h == last))
            def _():
                o_send.start()

            @pl.when(jnp.logical_and(second == 1, h == last))
            def _():
                o_store.start()

        early = (r - 1) * at_fin + u
        v = u - at_qz
        mid_slots = ends - at_qz
        w = u - (ends - 2)
        base = last * PIECES
        begin = jnp.where(r < n_heads, lax.div(early * PIECES, at_fin),
                          jnp.where(r == n_heads, base + lax.div(v * lags, mid_slots), base + lags + lax.div(w * PIECES, 4)))
        stop = jnp.where(r < n_heads, lax.div((early + 1) * PIECES, at_fin),
                         jnp.where(r == n_heads, base + lax.div((v + 1) * lags, mid_slots),
                                   base + lags + jnp.where(w == 0, PIECES // 4, PIECES)))
        live = jnp.logical_and(r > 0, r < n_heads + 2)

        def step(s, c):
            comm(s)
            return c
        lax.fori_loop(jnp.where(live, begin, 0), jnp.where(live, stop, 0), step, 0)

    def round_body(r, carry):
        lo = jnp.where(r < n_heads, 0, jnp.where(r == n_heads, at_qz, ends - 2))
        hi = jnp.where(r == 0, at_qz, jnp.where(r < n_heads, at_fin, ends))

        def one(u, c):
            slot_body(r, u)
            return c
        lax.fori_loop(lo, hi, one, 0)
        return carry
    lax.fori_loop(0, n_heads + 3, round_body, 0)

    x_send.wait_send()
    for o in range(1, nx):
        d_copy(o, x).wait_send()

    def drain(p, c):
        @pl.when(c_sends)
        def _():
            flow(0, c_out, c_in, p, down).wait_send()

        @pl.when(f_sends)
        def _():
            flow(1, f_out, f_in, p, right).wait_send()

        @pl.when(g_sends)
        def _():
            flow(2, g_out, g_in, p, left).wait_send()
        return c
    lax.fori_loop(0, total, drain, 0)
    o_store.wait()
    o_send.wait_send()
    pltpu.make_async_remote_copy(x_v.at[1 - core], out.at[1 - core], os_sem, or_sem, device_id=partner, device_id_type=MESH).wait_recv()


def solution(mesh):
    ny, nx = chip_grid(mesh.shape['sp'] // CORES)

    def device_body(hidden, w_in, w_gate, gate_bias, a_log, norm_w, w_out):
        _, rows, d_model = hidden.shape
        n_heads = w_gate.shape[1]
        val_dim = w_out.shape[0]
        key_dim = (w_in.shape[1] - 2 * val_dim) // 2
        head_k, head_v = key_dim // n_heads, val_dim // n_heads
        blk = head_k + head_v
        total = n_heads * PIECES
        any_space = pl.BlockSpec(memory_space=pl.ANY)
        vmem = pl.BlockSpec(memory_space=pltpu.VMEM)
        flow_buf = pltpu.VMEM((n_heads * head_k // 8, 8, head_v), F32)
        dma = pltpu.SemaphoreType.DMA
        return pl.pallas_call(
            functools.partial(layer_kernel, ny, nx),
            out_shape=jax.ShapeDtypeStruct(hidden.shape, BF16),
            in_specs=[any_space, any_space, vmem, vmem, vmem, vmem, any_space],
            out_specs=any_space,
            scratch_shapes=[
                pltpu.VMEM((2, rows, d_model), BF16),
                pltpu.VMEM((3, d_model, blk), BF16),
                pltpu.VMEM((2, head_v, w_out.shape[1]), BF16),
                pltpu.VMEM((128, d_model), BF16),
                pltpu.VMEM((16, 128), F32),
                pltpu.VMEM((2 * n_heads, 2, rows, blk), BF16),
                pltpu.VMEM((n_heads, 2, rows, head_v), F32),
                pltpu.VMEM((2, rows, w_out.shape[1]), F32),
                pltpu.VMEM((rows, head_v), BF16),
                pltpu.VMEM((2, rows, 128), F32),
                pltpu.VMEM((2, 128, rows), F32),
                pltpu.VMEM((2, rows, 128), F32),
                pltpu.VMEM((2, rows, 128), F32),
                pltpu.VMEM((8, 128), F32),
                pltpu.VMEM((nx, 8, 128), F32),
                pltpu.VMEM((4, n_heads, 8, head_v), F32),
                flow_buf, flow_buf, flow_buf, flow_buf, flow_buf, flow_buf, flow_buf,
                dma, dma, dma, dma((3, 2)), dma((2,)), dma((nx - 1,)), dma((nx - 1,)),
                dma((3, total)), dma((3, total)), dma, dma, dma,
            ],
            compiler_params=pltpu.CompilerParams(collective_id=0, has_side_effects=True, vmem_limit_bytes=67043328),
        )(hidden, w_in, w_gate.T, gate_bias.reshape(1, -1), a_log.reshape(1, -1), norm_w.reshape(1, -1), w_out)

    return jax.shard_map(device_body, mesh=mesh, in_specs=(P('dp', 'sp', None), P(), P(), P(), P(), P(), P()), out_specs=P('dp', 'sp', None), check_vma=False)
```
